32 devices in a mesh: pts: 8 (over z, y), grp: 4 (over x, core).
Axes of the slice: x: 2, y: 2, z: 4, core: 2. Of those that a mesh axis runs over, the one named last changes fastest.
Arguments:
- jacobian: bfloat16 [4096, 3, 3, 384], P(('pts', 'grp')), may hold values from -0.15625 to 0.15625
- owner: int32 [4096, 1], P(('pts', 'grp')), may hold values from 0 to 7; in each aligned block of 128 rows (0 to 127, 128 to 255, ...) at most 32 rows name the same one
- damping: float32 [8, 384], P('pts'), may hold values from 0.2 to 2
Outputs:
- reduced_diag: float32 [8, 384, 384], P('pts', None, 'grp')
- reduced_pair: float32 [8, 384, 384], P('pts', None, 'grp')
The draws below stay inside these ranges and needn't reach their ends.
Inputs may be any that keep to these rules, and one draw needn't show every extreme that they name: `owner`: among the 128 landmarks of one device at most 32 name the same segment, and in every draw some segment is named by exactly 32 landmarks of some device.
All inputs are finite; a program needn't handle non-finite values.
Results may differ from the reference program's by a relative error of at most 0.0003.
Values may be sent and summed in bfloat16 or wider, within the bound.
A program may use at most 64 MiB of HBM per device.

```python
import math
import jax
import jax.numpy as jnp
import numpy as np
from jax import lax

F = 384
PT = 128
CAP = 32
NE = 8
NPOINTS = 4096
N_PTS = 8
N_GRP = 4


def level_of(key, dims, cuts, low, top_value):
    def one(position, parts):
        steps = jax.random.uniform(jax.random.fold_in(jax.random.fold_in(key, 6), position), (parts,), jnp.float32, low / len(cuts), top_value / len(cuts))
        return jnp.repeat(jnp.exp(steps), dims[position] // parts).reshape((-1,) + (1,) * (len(dims) - position - 1))

    factor_of = one(*cuts[0])
    for cut in cuts[1:]:
        factor_of = factor_of * one(*cut)
    return factor_of


def assign_block(own_key, own, number, rows, amount, top, most, slope):
    order = jax.random.permutation(own_key, amount)
    heavy_load, usual = portions_of(amount, rows * top, most, slope, True), portions_of(amount, rows * top, most, slope, False)
    places = jnp.arange(amount)

    def named(sizes, offset_by):
        used = int((sizes > 0).sum())
        fixed = max(1, used // 4)
        moved = fixed + (places - fixed + offset_by * (used - fixed)) % max(1, amount - fixed)
        return jnp.zeros((amount,), jnp.int32).at[order[jnp.where(places < fixed, places, moved)]].set(jnp.asarray(sizes, jnp.int32))

    sizes = jnp.where(number % 4 == 0, named(heavy_load, number // 4), named(usual, number - number // 4 - 1))
    mixed = jax.random.permutation(jax.random.fold_in(own, 3), amount)
    source_of, sink = mixed[0:amount // 2 * 2:2], mixed[1:amount // 2 * 2:2]
    margin = jnp.minimum(sizes[source_of] - 1, most - sizes[sink]) // 2
    margin = jnp.where((source_of == order[0]) | (sink == order[0]) | (sizes[sink] == 0), 0, jnp.maximum(margin, 0))
    moved = jax.random.randint(jax.random.fold_in(own, 4), (amount // 2,), 0, 1 << 20) % (margin + 1)
    sizes = sizes.at[source_of].add(-moved).at[sink].add(moved)
    items = jnp.searchsorted(jnp.cumsum(sizes), jnp.arange(rows * top), side="right").astype(jnp.int32)
    table = items.reshape(top, rows).T
    table = table[jax.random.permutation(jax.random.fold_in(own, 1), rows)]
    offset_by = jax.random.randint(jax.random.fold_in(own, 2), (rows, 1), 0, top)
    return jnp.take_along_axis(table, (jnp.arange(top)[None, :] + offset_by) % top, axis=1)


def portions_of(amount, total, limit, slope, full):
    weights = [(1 << 20) // math.isqrt(grade ** slope) + 1 for grade in range(1, amount + 1)]
    largest = limit if full else min(limit, max(-(-total // amount), total * weights[0] // sum(weights)))
    least = 1 if total - largest >= amount - 1 else 0
    given, rest = [largest] + [least] * (amount - 1), total - largest - least * (amount - 1)
    while rest > 0:
        movable = [i for i in range(1, amount) if given[i] < largest] or [i for i in range(1, amount) if given[i] < limit]
        mass, budget = sum([weights[i] for i in movable]), rest
        for i in movable:
            extra = min(limit - given[i], max(1, budget * weights[i] // mass), rest)
            given[i] = given[i] + extra
            rest = rest - extra
    return np.array(given)


def bell_draw(rng, dims, spread, bound, split=(), held_as=jnp.bfloat16):
    values = jax.random.normal(rng, dims, jnp.float32) * spread
    if len(split) > 0:
        values = level_of(rng, dims, split, -0.22, 0.18) * values
    return jnp.clip(values, min=-bound, max=bound).astype(held_as)


def setup_inputs(seed: int = 0) -> dict:
    splits = jax.random.split(jax.random.key(seed), 4)
    jacobian = bell_draw(splits[0], (NPOINTS, 3, 3, F), (12 * PT) ** -0.5, 0.15625, ((0, 32),))
    owner_keys = jax.random.split(jax.random.fold_in(splits[1], 1), NPOINTS // PT)
    owner_turns = jax.random.permutation(jax.random.fold_in(splits[1], 3), NPOINTS // PT)
    owner = jax.vmap(lambda own, number: assign_block(jax.random.fold_in(splits[1], 2), own, number, PT, N_PTS, 1, CAP, 2))(owner_keys, owner_turns).reshape((NPOINTS, 1))
    damping = jnp.clip(jnp.exp(math.log(2.0) - 2.3025851 * jax.random.uniform(splits[2], (NE, F), jnp.float32) ** level_of(splits[2], (NE, F), ((0, 8),), -0.2, 0.2)), 0.2, 2.0)
    return {"jacobian": jacobian, "owner": owner, "damping": damping}


def gram(left, right):
    return lax.dot_general(left.astype(jnp.float32), right.astype(jnp.float32), (((0,), (0,)), ((), ())), preferred_element_type=jnp.float32)

def exact_gram(left, right):
    return lax.dot_general(left.astype(jnp.float32), right.astype(jnp.float32), (((0,), (0,)), ((), ())), precision=lax.Precision.HIGHEST, preferred_element_type=jnp.float32)

def reference(jacobian, owner, damping):
    window = N_PTS * N_GRP * CAP
    width = jacobian.shape[3]
    segment = owner[:, 0].astype(jnp.int32)
    order = jnp.argsort(segment, stable=True)
    sorted_rows = jacobian[order]
    counts = jax.ops.segment_sum(jnp.ones_like(segment), segment, num_segments=NE).astype(jnp.int32)
    starts = (jnp.cumsum(counts) - counts).astype(jnp.int32)
    padded = jnp.concatenate([sorted_rows, jnp.zeros((window, 3, 3, width), jacobian.dtype)], 0)

    def one_segment(items):
        start, count, lm_row = items
        rows = lax.dynamic_slice_in_dim(padded, start.astype(jnp.int32), window, 0)
        keep = jnp.arange(window, dtype=jnp.int32) < count
        rows = jnp.where(keep[:, None, None, None], rows, jnp.zeros_like(rows))
        first = rows[:, 0].reshape(window * 3, width)
        middle = rows[:, 1].reshape(window * 3, width)
        last = rows[:, 2].reshape(window * 3, width)
        d_low = gram(first, first)
        d_odd = gram(middle, middle)
        d_high = gram(last, last)
        b_low = gram(middle, first)
        b_high = gram(middle, last)
        e_pair = gram(first, last)
        system = d_odd + jnp.diag(lm_row)
        factor = jnp.linalg.cholesky(system)
        y_low = lax.linalg.triangular_solve(factor, b_low, left_side=True, lower=True)
        y_high = lax.linalg.triangular_solve(factor, b_high, left_side=True, lower=True)
        low = d_low - exact_gram(y_low, y_low)
        high = d_high - exact_gram(y_high, y_high)
        pair = e_pair - exact_gram(y_low, y_high)
        return (low, high, pair)
    low, high, pair = lax.map(one_segment, (starts, counts, damping))
    reduced_diag = low + jnp.roll(high, 1, axis=0)
    return (reduced_diag, pair)
```

```python
import functools

import jax
import jax.numpy as jnp
from jax import lax
from jax.experimental import pallas as pl
from jax.experimental.pallas import tpu as pltpu
from jax.sharding import PartitionSpec as P

MESH = pl.DeviceIdType.MESH
LANES = 128
TILE = 8
PANEL = 32


def mm(left, right, dims, precise):
    return lax.dot_general(
        left,
        right,
        (dims, ((), ())),
        precision=lax.Precision.HIGHEST if precise else None,
        preferred_element_type=jnp.float32,
    )


NN = ((1,), (0,))
NT = ((1,), (1,))
TN = ((0,), (0,))


def sub_row(tile, r):
    return jnp.broadcast_to(tile[r : r + 1, :], (TILE, LANES))


def sub_lane(tile, c):
    return jnp.broadcast_to(tile[:, c : c + 1], (TILE, LANES))


def invert_panel(tiles, first, group):
    lane = lax.broadcasted_iota(jnp.int32, (TILE, LANES), 1)
    sub = lax.broadcasted_iota(jnp.int32, (TILE, LANES), 0)
    count = len(tiles)
    for tile in range(count):
        start = tile * TILE
        columns = {u: [sub_lane(row[group], first + start + u) for row in tiles] for u in range(TILE)}
        for t in range(TILE):
            at = first + start + t
            here = sub == t
            pivot = columns.pop(t)
            scale = 1.0 / sub_row(pivot[tile], t)
            for u in columns:
                lead = sub_row(columns[u][tile], t) * scale
                columns[u] = [c - p * lead for c, p in zip(columns[u], pivot)]
                columns[u][tile] = jnp.where(here, lead, columns[u][tile])
            for part in range(len(tiles[0])):
                row = sub_row(tiles[tile][part], t) * scale
                if part == group:
                    row = jnp.where(lane == at, scale, row)
                for g in range(count):
                    old = tiles[g][part]
                    if part == group:
                        old = jnp.where(lane == at, 0.0, old)
                    tiles[g][part] = old - pivot[g] * row
                tiles[tile][part] = jnp.where(here, row, tiles[tile][part])
    return tiles


def invert(s, between):
    size = s.shape[0]
    panels = size // PANEL
    lane = lax.broadcasted_iota(jnp.int32, (1, size), 1)

    def tiles_of(value):
        return [
            [value[g : g + TILE, c : c + LANES] for c in range(0, size, LANES)]
            for g in range(0, PANEL, TILE)
        ]

    def updated(j, rows):
        at = slice(j * PANEL, (j + 1) * PANEL)
        kept = jnp.where((lane >= j * PANEL) & (lane < (j + 1) * PANEL), 0.0, s[rows, :])
        return kept - mm(s[rows, at], s[at, :], NN, True)

    def update(j, after):
        for rows in (slice(0, j * PANEL), slice((j + after) * PANEL, size)):
            if rows.stop > rows.start:
                s[rows, :] = updated(j, rows)

    tiles = tiles_of(s[:PANEL, :])
    for j in range(panels):
        between(j)
        if j:
            update(j - 1, 2)
        tiles = invert_panel(tiles, j * PANEL % LANES, j * PANEL // LANES)
        for g in range(PANEL // TILE):
            for c in range(size // LANES):
                s[j * PANEL + g * TILE : j * PANEL + (g + 1) * TILE, c * LANES : (c + 1) * LANES] = tiles[g][c]
        if j + 1 < panels:
            tiles = tiles_of(updated(j, slice((j + 1) * PANEL, (j + 2) * PANEL)))
    update(panels - 1, 1)


def kernel(
    owners, groups, rows_per, width, capacity,
    planes, owner_row, damp, low_out, pair_out, carried,
    send, recv, sblk, s1, s2, system, gram, r1, r2, bt, highs,
    a_send, a_recv, d_send, d_recv, d2_recv, g_send, g_recv, b_send, b_recv, c_send, c_recv, own_sem,
):
    me = lax.axis_index("pts")
    grp = lax.axis_index("grp")
    near = grp + 1 - 2 * lax.rem(grp, 2)
    far = lax.rem(grp + 2, groups)
    chunk = width // groups
    nb = width // LANES
    pairs = [(i, j) for i in range(nb) for j in range(i, nb)]
    odd = lax.rem(grp, 2)

    barrier = pltpu.get_barrier_semaphore()

    def greet(off, _):
        pl.semaphore_signal(
            barrier, inc=1, device_id=(lax.rem(me + off, owners), grp), device_id_type=MESH
        )
        return 0

    lax.fori_loop(1, owners, greet, 0)
    for other in (near, far):
        pl.semaphore_signal(barrier, inc=1, device_id=(me, other), device_id_type=MESH)

    clusters, spots, _ = planes.shape
    points = owner_row.shape[1]
    earlier = (
        lax.broadcasted_iota(jnp.int32, (points, points), 0)
        < lax.broadcasted_iota(jnp.int32, (points, points), 1)
    )
    spread = jnp.broadcast_to(owner_row[...], (points, points))
    ahead = jnp.where((spread.T == spread) & earlier, 1, 0)
    place = owner_row[...] * rows_per + jnp.sum(ahead, axis=0, keepdims=True)
    place = jnp.concatenate([place + capacity * r for r in range(spots // points)], 1)
    slot = lax.broadcasted_iota(jnp.int32, (owners * rows_per, spots), 0)
    pick = jnp.where(slot == place, 1.0, 0.0).astype(send.dtype)

    def pack(k):
        send[k] = mm(pick, planes[k], NN, False).astype(send.dtype)

    pack(1)
    pl.semaphore_wait(barrier, owners - 1 + 2)

    def rows_at(i):
        return pl.ds(pl.multiple_of(i * rows_per, rows_per), rows_per)

    for k in (1, 0, 2):
        if k != 1:
            pack(k)

        def issue(off, _, k=k):
            to = lax.rem(me + off, owners)
            pltpu.make_async_remote_copy(
                src_ref=send.at[k, rows_at(to)],
                dst_ref=recv.at[k, rows_at(me)],
                send_sem=a_send.at[k],
                recv_sem=a_recv.at[k],
                device_id=(to, grp),
                device_id_type=MESH,
            ).start()
            return 0

        lax.fori_loop(1, owners, issue, 0)
    for k in range(3):
        pltpu.make_async_copy(
            send.at[k, rows_at(me)], recv.at[k, rows_at(me)], own_sem.at[k]
        ).start()
    for k in range(3):
        pltpu.make_async_copy(
            send.at[k, rows_at(me)], recv.at[k, rows_at(me)], own_sem.at[k]
        ).wait()

    def await_rows(k):
        part = recv.at[k, pl.ds(0, (owners - 1) * rows_per)]
        pltpu.make_async_copy(part, part, a_recv.at[k]).wait()

    await_rows(1)
    first_copies = []
    own = len(pairs)
    for i in range(nb):
        strip = mm(
            recv[1, :, i * LANES : (i + 1) * LANES], recv[1, :, i * LANES :], TN, False
        )
        for j in range(i, nb):
            n = pairs.index((i, j))
            sblk[n] = strip[:, (j - i) * LANES : (j - i + 1) * LANES]
            copy = pltpu.make_async_remote_copy(
                src_ref=sblk.at[n], dst_ref=s1.at[n],
                send_sem=d_send.at[n], recv_sem=d_recv.at[n],
                device_id=(me, near), device_id_type=MESH,
            )
            copy.start()
            first_copies.append(copy)
    second_copies = []

    def forward(some):
        for n in some:
            first_copies[n].wait_recv()
            sblk[own + n] = sblk[n] + s1[n]
            copy = pltpu.make_async_remote_copy(
                src_ref=sblk.at[own + n], dst_ref=s2.at[n],
                send_sem=d_send.at[own + n], recv_sem=d2_recv.at[n],
                device_id=(me, far), device_id_type=MESH,
            )
            copy.start()
            second_copies.append(copy)

    forward(range(1))

    eye = (
        lax.broadcasted_iota(jnp.int32, (LANES, LANES), 0)
        == lax.broadcasted_iota(jnp.int32, (LANES, LANES), 1)
    )

    def reduced(n):
        second_copies[n].wait_recv()
        i, j = pairs[n]
        total = sblk[own + n] + s2[n]
        if i == j:
            total = total + jnp.where(eye, damp[:, i * LANES : (i + 1) * LANES], 0.0)
        return total

    sides = ((0, 1), (2, 1), (0, 0), (2, 2), (2, 0))

    def chunk_rows(c):
        return pl.ds(pl.multiple_of(c * chunk, TILE), chunk)

    def near_copy(m, h):
        return pltpu.make_async_remote_copy(
            src_ref=gram.at[m, chunk_rows(1 - odd + 2 * h)], dst_ref=r1.at[m, h],
            send_sem=g_send.at[m, h], recv_sem=g_recv.at[m, h],
            device_id=(me, near), device_id_type=MESH,
        )

    def far_copy(m, h):
        return pltpu.make_async_remote_copy(
            src_ref=gram.at[m, chunk_rows(odd + 2 * h if m < 2 else far)], dst_ref=r2.at[m, h],
            send_sem=g_send.at[m, 2 + h], recv_sem=g_recv.at[m, 2 + h],
            device_id=(me, far), device_id_type=MESH,
        )

    def spread_near(m, h):
        at = chunk_rows(odd + 2 * h)
        return pltpu.make_async_remote_copy(
            src_ref=bt.at[m, at], dst_ref=bt.at[m, at],
            send_sem=b_send.at[m, h], recv_sem=b_recv.at[m, h],
            device_id=(me, near), device_id_type=MESH,
        )

    def far_parts(m):
        return range(2) if m < 2 else range(1)

    def make_grams(k, some):
        await_rows(k)
        for m in some:
            left, right = sides[m]
            gram[m] = mm(recv[left], recv[right], TN, False)
            for h in range(2):
                near_copy(m, h).start()

    def fold_near(some):
        for m in some:
            for h in range(2):
                near_copy(m, h).wait()
                at = chunk_rows(odd + 2 * h)
                gram[m, at, :] = gram[m, at, :] + r1[m, h]
            for h in far_parts(m):
                far_copy(m, h).start()

    def fold_far(m):
        for h in far_parts(m):
            far_copy(m, h).wait()
            if m < 2:
                at = chunk_rows(odd + 2 * h)
                bt[m, at, :] = gram[m, at, :] + r2[m, h]
                spread_near(m, h).start()
            else:
                at = chunk_rows(grp)
                gram[m, at, :] = gram[m, at, :] + r2[m, h]

    def second_near():
        fold_near((1,))
        fold_far(0)

    forward(range(1, own))
    for n, (i, j) in enumerate(pairs):
        total = reduced(n)
        ri, rj = slice(i * LANES, (i + 1) * LANES), slice(j * LANES, (j + 1) * LANES)
        system[ri, rj] = total
        if i != j:
            system[rj, ri] = total.T

    hooks = {
        1: functools.partial(make_grams, 0, (0, 2)),
        2: functools.partial(fold_near, (0,)),
        3: functools.partial(fold_near, (2,)),
        8: functools.partial(make_grams, 2, (1, 3, 4)),
        9: second_near,
        10: functools.partial(fold_near, (3,)),
        11: functools.partial(fold_near, (4,)),
    }

    def between(j):
        if j in hooks:
            hooks.pop(j)()

    invert(system, between)
    for key in sorted(hooks):
        hooks[key]()
    mine = chunk_rows(grp)

    def eliminate(m):
        for h in range(2):
            spread_near(m, h).wait()
        return mm(bt[m, mine, :], system[...], NN, True)

    fold_far(1)
    solved_low = eliminate(0)
    fold_far(2)
    low_out[...] = gram[2, mine, :] - mm(solved_low, bt[0], NT, True)
    solved_high = eliminate(1)
    fold_far(3)
    highs[...] = gram[3, mine, :] - mm(solved_high, bt[1], NT, True)
    carry = pltpu.make_async_remote_copy(
        src_ref=highs, dst_ref=carried, send_sem=c_send, recv_sem=c_recv,
        device_id=(lax.rem(me + 1, owners), grp), device_id_type=MESH,
    )
    carry.start()
    fold_far(4)
    pair_out[...] = gram[4, mine, :] - mm(solved_high, bt[0], NT, True)
    for copy in first_copies + second_copies:
        copy.wait_send()
    for k in range(3):
        part = send.at[k, pl.ds(0, (owners - 1) * rows_per)]
        pltpu.make_async_copy(part, part, a_send.at[k]).wait()
    carry.wait()


def finish(low, pair, carried, diag_out, pair_out):
    diag_out[...] = low[...] + carried[...]
    pair_out[...] = pair[...]


def local(jacobian, owner, damping):
    points, clusters, residuals, width = jacobian.shape
    owners = lax.axis_size("pts")
    groups = lax.axis_size("grp")
    capacity = max(2, 2 * points // owners)
    rows_per = -(-residuals * capacity // 16) * 16
    total = owners * rows_per
    planes = jnp.transpose(jacobian, (1, 2, 0, 3)).reshape(clusters, residuals * points, width)
    chunk = width // groups
    nb = width // LANES
    blocks = nb * (nb + 1) // 2
    vmem = pl.BlockSpec(memory_space=pltpu.VMEM)
    dma = pltpu.SemaphoreType.DMA
    low, pair, carried = pl.pallas_call(
        functools.partial(kernel, owners, groups, rows_per, width, capacity),
        out_shape=[jax.ShapeDtypeStruct((chunk, width), jnp.float32)] * 3,
        in_specs=[vmem] * 3,
        out_specs=[vmem] * 3,
        scratch_shapes=[
            pltpu.VMEM((clusters, total, width), jacobian.dtype),
            pltpu.VMEM((clusters, total, width), jacobian.dtype),
            pltpu.VMEM((2 * blocks, LANES, LANES), jnp.float32),
            pltpu.VMEM((blocks, LANES, LANES), jnp.float32),
            pltpu.VMEM((blocks, LANES, LANES), jnp.float32),
            pltpu.VMEM((width, width), jnp.float32),
            pltpu.VMEM((5, width, width), jnp.float32),
            pltpu.VMEM((5, 2, chunk, width), jnp.float32),
            pltpu.VMEM((5, 2, chunk, width), jnp.float32),
            pltpu.VMEM((2, width, width), jnp.float32),
            pltpu.VMEM((chunk, width), jnp.float32),
            dma((3,)), dma((3,)),
            dma((2 * blocks,)), dma((blocks,)), dma((blocks,)),
            dma((5, 4)), dma((5, 4)),
            dma((2, 2)), dma((2, 2)),
            dma, dma, dma((3,)),
        ],
        compiler_params=pltpu.CompilerParams(collective_id=0, has_side_effects=True),
    )(planes, owner.reshape(1, points), damping)
    diag, pair = pl.pallas_call(
        finish,
        out_shape=[jax.ShapeDtypeStruct((chunk, width), jnp.float32)] * 2,
        in_specs=[vmem] * 3,
        out_specs=[vmem] * 2,
    )(low, pair, carried)
    return diag.T[None], pair.T[None]


def solution(mesh):
    placed = (P(("pts", "grp"), None, None, None), P(("pts", "grp"), None), P("pts", None))
    return jax.shard_map(
        local,
        mesh=mesh,
        in_specs=placed,
        out_specs=(P("pts", None, "grp"), P("pts", None, "grp")),
        check_vma=False,
    )
```

```python
import functools

import jax
import jax.numpy as jnp
from jax import lax
from jax.experimental import pallas as pl
from jax.experimental.pallas import tpu as pltpu
from jax.sharding import PartitionSpec as P

MESH = pl.DeviceIdType.MESH
LANES = 128
TILE = 8
PANEL = 32
BATCHES = 8


def mm(left, right, dims, precise):
    return lax.dot_general(
        left,
        right,
        (dims, ((), ())),
        precision=lax.Precision.HIGHEST if precise else None,
        preferred_element_type=jnp.float32,
    )


NN = ((1,), (0,))
NT = ((1,), (1,))
TN = ((0,), (0,))


def sub_row(tile, r):
    return jnp.broadcast_to(tile[r : r + 1, :], (TILE, LANES))


def sub_lane(tile, c):
    return jnp.broadcast_to(tile[:, c : c + 1], (TILE, LANES))


def invert_panel(tiles, first, group):
    lane = lax.broadcasted_iota(jnp.int32, (TILE, LANES), 1)
    sub = lax.broadcasted_iota(jnp.int32, (TILE, LANES), 0)
    count = len(tiles)
    for tile in range(count):
        start = tile * TILE
        columns = {u: [sub_lane(row[group], first + start + u) for row in tiles] for u in range(TILE)}
        for t in range(TILE):
            at = first + start + t
            here = sub == t
            pivot = columns.pop(t)
            scale = 1.0 / sub_row(pivot[tile], t)
            for u in columns:
                lead = sub_row(columns[u][tile], t) * scale
                columns[u] = [c - p * lead for c, p in zip(columns[u], pivot)]
                columns[u][tile] = jnp.where(here, lead, columns[u][tile])
            for part in range(len(tiles[0])):
                row = sub_row(tiles[tile][part], t) * scale
                if part == group:
                    row = jnp.where(lane == at, scale, row)
                for g in range(count):
                    old = tiles[g][part]
                    if part == group:
                        old = jnp.where(lane == at, 0.0, old)
                    tiles[g][part] = old - pivot[g] * row
                tiles[tile][part] = jnp.where(here, row, tiles[tile][part])
    return tiles


def invert(s, between):
    size = s.shape[0]
    panels = size // PANEL
    lane = lax.broadcasted_iota(jnp.int32, (1, size), 1)

    def tiles_of(value):
        return [
            [value[g : g + TILE, c : c + LANES] for c in range(0, size, LANES)]
            for g in range(0, PANEL, TILE)
        ]

    def updated(j, rows):
        at = slice(j * PANEL, (j + 1) * PANEL)
        kept = jnp.where((lane >= j * PANEL) & (lane < (j + 1) * PANEL), 0.0, s[rows, :])
        return kept - mm(s[rows, at], s[at, :], NN, True)

    def update(j, after):
        for rows in (slice(0, j * PANEL), slice((j + after) * PANEL, size)):
            if rows.stop > rows.start:
                s[rows, :] = updated(j, rows)

    tiles = tiles_of(s[:PANEL, :])
    for j in range(panels):
        between(j)
        if j:
            update(j - 1, 2)
        tiles = invert_panel(tiles, j * PANEL % LANES, j * PANEL // LANES)
        for g in range(PANEL // TILE):
            for c in range(size // LANES):
                s[j * PANEL + g * TILE : j * PANEL + (g + 1) * TILE, c * LANES : (c + 1) * LANES] = tiles[g][c]
        if j + 1 < panels:
            tiles = tiles_of(updated(j, slice((j + 1) * PANEL, (j + 2) * PANEL)))
    update(panels - 1, 1)


def partner(me, r, owners):
    out, bit = 0, 1
    while bit < owners:
        mine, flip = lax.rem(me // bit, 2), (r // bit) % 2
        out = out + bit * (mine + flip - 2 * mine * flip)
        bit *= 2
    return out


def kernel(
    owners, groups, rows_per, width, capacity,
    planes, owner_row, damp, low_out, pair_out, carried,
    send, rows, system, part, other, window, chunks, highs,
    a_send, a_recv, own_sem, f_send, f_recv, n_send, n_recv, w_send, w_recv, c_send, c_recv,
):
    me = lax.axis_index("pts")
    grp = lax.axis_index("grp")
    near = grp + 1 - 2 * lax.rem(grp, 2)
    far = lax.rem(grp + 2, groups)
    chunk = width // groups
    nb = width // LANES
    batches = min(owners, BATCHES)
    units = owners // batches
    unit_rows = units * rows_per

    barrier = pltpu.get_barrier_semaphore()

    def greet(r, _):
        pl.semaphore_signal(
            barrier, inc=1, device_id=(partner(me, r, owners), grp), device_id_type=MESH
        )
        return 0

    lax.fori_loop(1, owners, greet, 0)
    for peer in (near, far):
        pl.semaphore_signal(barrier, inc=1, device_id=(me, peer), device_id_type=MESH)

    clusters, spots, _ = planes.shape
    points = owner_row.shape[1]
    earlier = (
        lax.broadcasted_iota(jnp.int32, (points, points), 0)
        < lax.broadcasted_iota(jnp.int32, (points, points), 1)
    )
    spread = jnp.broadcast_to(owner_row[...], (points, points))
    ahead = jnp.where((spread.T == spread) & earlier, 1, 0)
    place = owner_row[...] * rows_per + jnp.sum(ahead, axis=0, keepdims=True)
    place = jnp.concatenate([place + capacity * r for r in range(spots // points)], 1)
    slot = lax.broadcasted_iota(jnp.int32, (owners * rows_per, spots), 0)
    pick = jnp.where(slot == place, 1.0, 0.0).astype(send.dtype)

    def pack(k):
        send[k] = mm(pick, planes[k], NN, False).astype(send.dtype)

    def rows_at(i):
        return pl.ds(pl.multiple_of(i * rows_per, rows_per), rows_per)

    def landing(b, side):
        return pl.ds((2 * b + side) * unit_rows, unit_rows)

    def own_copy(k):
        return pltpu.make_async_copy(
            send.at[k, rows_at(me)], rows.at[k, pl.ds(0, rows_per)], own_sem.at[k]
        )

    def issue(k, b):
        def one(i, _):
            r = b * units + i
            to = partner(me, r, owners)
            at = 2 * b * unit_rows + i * rows_per
            pltpu.make_async_remote_copy(
                src_ref=send.at[k, rows_at(to)],
                dst_ref=rows.at[k, pl.ds(pl.multiple_of(at, rows_per), rows_per)],
                send_sem=a_send.at[k], recv_sem=a_recv.at[k, b],
                device_id=(to, grp), device_id_type=MESH,
            ).start()
            return 0

        if b == 0:
            own_copy(k).start()
        if units == 1:
            if b:
                one(0, 0)
        else:
            lax.fori_loop(0 if b else 1, units, one, 0)

    far_copies = {}

    def arrive(k, b):
        remote = unit_rows if b else unit_rows - rows_per
        if remote:
            taken = rows.at[k, pl.ds(0, remote)]
            pltpu.make_async_copy(taken, taken, a_recv.at[k, b]).wait()
        if b == 0:
            own_copy(k).wait()
        copy = pltpu.make_async_remote_copy(
            src_ref=rows.at[k, landing(b, 0)], dst_ref=rows.at[k, landing(b, 1)],
            send_sem=f_send.at[k, b], recv_sem=f_recv.at[k, b],
            device_id=(me, far), device_id_type=MESH,
        )
        copy.start()
        far_copies[k, b] = copy

    def landed(k, some):
        for b in some:
            far_copies[k, b].wait_recv()

    def span(some):
        return slice(2 * some[0] * unit_rows, 2 * (some[-1] + 1) * unit_rows)

    half = -(-2 * chunk // LANES) * LANES
    start = pl.multiple_of(grp // 2 * (width - half), LANES)

    def add_full(n, left, right, some):
        value = mm(rows[left, span(some), :], rows[right, span(some), :], TN, False)
        part[n] = value if some[0] == 0 else part[n] + value

    def add_window(m, left, right, some):
        value = mm(
            rows[left, span(some), pl.ds(start, half)], rows[right, span(some), :], TN, False
        )
        window[m] = value if some[0] == 0 else window[m] + value

    def full_copy(n):
        return pltpu.make_async_remote_copy(
            src_ref=part.at[n], dst_ref=other.at[n],
            send_sem=n_send.at[n], recv_sem=n_recv.at[n],
            device_id=(me, near), device_id_type=MESH,
        )

    def in_window(g):
        return pl.ds(pl.multiple_of(g * chunk - start, TILE), chunk)

    def window_copy(m):
        return pltpu.make_async_remote_copy(
            src_ref=window.at[m, in_window(near)], dst_ref=chunks.at[m],
            send_sem=w_send.at[m], recv_sem=w_recv.at[m],
            device_id=(me, near), device_id_type=MESH,
        )

    mine = pl.ds(pl.multiple_of(grp * chunk, TILE), chunk)

    def summed(n):
        full_copy(n).wait()
        other[n] = part[n] + other[n]

    def own_chunk(m):
        window_copy(m).wait()
        return window[m, in_window(grp), :] + chunks[m]

    pack(1)
    pl.semaphore_wait(barrier, owners - 1 + 2)
    everything = list(range(batches))
    early, late = everything[: batches // 2], everything[batches // 2 :]
    for b in everything:
        issue(1, b)
    pack(2)
    for b in early:
        arrive(1, b)
        issue(2, b)
    pack(0)
    arrive(2, 0)
    issue(0, 0)
    for b in late:
        arrive(1, b)
        issue(2, b)
        if b == late[0]:
            landed(1, early)
            add_full(0, 1, 1, early)
        if b - len(early) + 1 in early:
            arrive(2, b - len(early) + 1)
            issue(0, b - len(early) + 1)
    landed(1, late)
    add_full(0, 1, 1, late)
    full_copy(0).start()
    full_copy(0).wait()
    eye = (
        lax.broadcasted_iota(jnp.int32, (LANES, LANES), 0)
        == lax.broadcasted_iota(jnp.int32, (LANES, LANES), 1)
    )
    system[...] = part[0] + other[0]
    for i in range(nb):
        at = slice(i * LANES, (i + 1) * LANES)
        system[at, at] = system[at, at] + jnp.where(eye, damp[:, at], 0.0)

    def grams_high():
        landed(2, everything)
        add_full(1, 2, 1, everything)
        full_copy(1).start()
        add_window(0, 2, 2, everything)
        window_copy(0).start()

    plan = {
        0: [(2, late[0])], 1: [(0, 0)], 2: [(2, late[1])], 3: [(0, 1)], 4: [(2, late[2])],
        5: [(0, 2)], 6: [(2, late[3])], 7: [(0, 3)], 9: [(0, late[0])], 11: [(0, late[1])],
    }

    def between(j):
        for k, b in plan.get(j, ()):
            arrive(k, b)
            if k == 2:
                issue(0, b)
        if j == 10:
            grams_high()

    invert(system, between)
    summed(1)
    solved_high = mm(other[1, mine, :], system[...], NN, True)
    arrive(0, late[2])
    highs[...] = own_chunk(0) - mm(solved_high, other[1], NT, True)
    carry = pltpu.make_async_remote_copy(
        src_ref=highs, dst_ref=carried, send_sem=c_send, recv_sem=c_recv,
        device_id=(lax.rem(me + 1, owners), grp), device_id_type=MESH,
    )
    carry.start()
    arrive(0, late[3])
    first = everything[:-1]
    for some in (first, everything[-1:]):
        landed(0, some)
        add_full(2, 0, 1, some)
        if some is not first:
            full_copy(2).start()
        add_window(1, 0, 0, some)
        add_window(2, 2, 0, some)
    window_copy(1).start()
    window_copy(2).start()
    summed(2)
    solved_low = mm(other[2, mine, :], system[...], NN, True)
    low_out[...] = own_chunk(1) - mm(solved_low, other[2], NT, True)
    pair_out[...] = own_chunk(2) - mm(solved_high, other[2], NT, True)
    for copy in far_copies.values():
        copy.wait_send()
    for k in range(clusters):
        sent = send.at[k, pl.ds(0, (owners - 1) * rows_per)]
        pltpu.make_async_copy(sent, sent, a_send.at[k]).wait()
    carry.wait()


def finish(low, pair, carried, diag_out, pair_out):
    diag_out[...] = low[...] + carried[...]
    pair_out[...] = pair[...]


def local(jacobian, owner, damping):
    points, clusters, residuals, width = jacobian.shape
    owners = lax.axis_size("pts")
    groups = lax.axis_size("grp")
    capacity = max(2, 2 * points // owners)
    rows_per = -(-residuals * capacity // 16) * 16
    total = owners * rows_per
    planes = jnp.transpose(jacobian, (1, 2, 0, 3)).reshape(clusters, residuals * points, width)
    chunk = width // groups
    half = -(-2 * chunk // LANES) * LANES
    batches = min(owners, BATCHES)
    vmem = pl.BlockSpec(memory_space=pltpu.VMEM)
    dma = pltpu.SemaphoreType.DMA
    low, pair, carried = pl.pallas_call(
        functools.partial(kernel, owners, groups, rows_per, width, capacity),
        out_shape=[jax.ShapeDtypeStruct((chunk, width), jnp.float32)] * 3,
        in_specs=[vmem] * 3,
        out_specs=[vmem] * 3,
        scratch_shapes=[
            pltpu.VMEM((clusters, total, width), jacobian.dtype),
            pltpu.VMEM((clusters, 2 * total, width), jacobian.dtype),
            pltpu.VMEM((width, width), jnp.float32),
            pltpu.VMEM((3, width, width), jnp.float32),
            pltpu.VMEM((3, width, width), jnp.float32),
            pltpu.VMEM((3, half, width), jnp.float32),
            pltpu.VMEM((3, chunk, width), jnp.float32),
            pltpu.VMEM((chunk, width), jnp.float32),
            dma((clusters,)), dma((clusters, batches)), dma((clusters,)),
            dma((clusters, batches)), dma((clusters, batches)),
            dma((3,)), dma((3,)), dma((3,)), dma((3,)),
            dma, dma,
        ],
        compiler_params=pltpu.CompilerParams(collective_id=0, has_side_effects=True),
    )(planes, owner.reshape(1, points), damping)
    diag, pair = pl.pallas_call(
        finish,
        out_shape=[jax.ShapeDtypeStruct((chunk, width), jnp.float32)] * 2,
        in_specs=[vmem] * 3,
        out_specs=[vmem] * 2,
    )(low, pair, carried)
    return diag.T[None], pair.T[None]


def solution(mesh):
    placed = (P(("pts", "grp"), None, None, None), P(("pts", "grp"), None), P("pts", None))
    return jax.shard_map(
        local,
        mesh=mesh,
        in_specs=placed,
        out_specs=(P("pts", None, "grp"), P("pts", None, "grp")),
        check_vma=False,
    )
```

```python
import functools

import jax
import jax.numpy as jnp
from jax import lax
from jax.experimental import pallas as pl
from jax.experimental.pallas import tpu as pltpu
from jax.sharding import PartitionSpec as P

MESH = pl.DeviceIdType.MESH
LANES = 128
TILE = 8
PANEL = 32
BATCHES = 8


def mm(left, right, dims, precise):
    return lax.dot_general(
        left,
        right,
        (dims, ((), ())),
        precision=lax.Precision.HIGHEST if precise else None,
        preferred_element_type=jnp.float32,
    )


NN = ((1,), (0,))
NT = ((1,), (1,))
TN = ((0,), (0,))


def sub_row(tile, r):
    return jnp.broadcast_to(tile[r : r + 1, :], (TILE, LANES))


def sub_lane(tile, c):
    return jnp.broadcast_to(tile[:, c : c + 1], (TILE, LANES))


def invert_panel(tiles, first, group):
    lane = lax.broadcasted_iota(jnp.int32, (TILE, LANES), 1)
    sub = lax.broadcasted_iota(jnp.int32, (TILE, LANES), 0)
    count = len(tiles)
    for tile in range(count):
        start = tile * TILE
        columns = {u: [sub_lane(row[group], first + start + u) for row in tiles] for u in range(TILE)}
        for t in range(TILE):
            at = first + start + t
            here = sub == t
            pivot = columns.pop(t)
            scale = 1.0 / sub_row(pivot[tile], t)
            for u in columns:
                lead = sub_row(columns[u][tile], t) * scale
                columns[u] = [c - p * lead for c, p in zip(columns[u], pivot)]
                columns[u][tile] = jnp.where(here, lead, columns[u][tile])
            for part in range(len(tiles[0])):
                row = sub_row(tiles[tile][part], t) * scale
                if part == group:
                    row = jnp.where(lane == at, scale, row)
                for g in range(count):
                    old = tiles[g][part]
                    if part == group:
                        old = jnp.where(lane == at, 0.0, old)
                    tiles[g][part] = old - pivot[g] * row
                tiles[tile][part] = jnp.where(here, row, tiles[tile][part])
    return tiles


def invert(s, between):
    size = s.shape[0]
    panels = size // PANEL
    lane = lax.broadcasted_iota(jnp.int32, (1, size), 1)

    def tiles_of(value):
        return [
            [value[g : g + TILE, c : c + LANES] for c in range(0, size, LANES)]
            for g in range(0, PANEL, TILE)
        ]

    def updated(j, rows):
        at = slice(j * PANEL, (j + 1) * PANEL)
        kept = jnp.where((lane >= j * PANEL) & (lane < (j + 1) * PANEL), 0.0, s[rows, :])
        return kept - mm(s[rows, at], s[at, :], NN, True)

    def update(j, after):
        for rows in (slice(0, j * PANEL), slice((j + after) * PANEL, size)):
            if rows.stop > rows.start:
                s[rows, :] = updated(j, rows)

    tiles = tiles_of(s[:PANEL, :])
    for j in range(panels):
        between(j)
        if j:
            update(j - 1, 2)
        tiles = invert_panel(tiles, j * PANEL % LANES, j * PANEL // LANES)
        for g in range(PANEL // TILE):
            for c in range(size // LANES):
                s[j * PANEL + g * TILE : j * PANEL + (g + 1) * TILE, c * LANES : (c + 1) * LANES] = tiles[g][c]
        if j + 1 < panels:
            tiles = tiles_of(updated(j, slice((j + 1) * PANEL, (j + 2) * PANEL)))
    update(panels - 1, 1)


def partner(me, r, owners):
    out, bit = 0, 1
    while bit < owners:
        mine, flip = lax.rem(me // bit, 2), (r // bit) % 2
        out = out + bit * (mine + flip - 2 * mine * flip)
        bit *= 2
    return out


def kernel(
    owners, groups, rows_per, width, capacity,
    planes, owner_row, damp, low_out, pair_out, carried,
    send, rows, system, part, other, window, chunks, highs,
    a_send, a_recv, own_sem, f_send, f_recv, n_send, n_recv, w_send, w_recv, c_send, c_recv,
):
    me = lax.axis_index("pts")
    grp = lax.axis_index("grp")
    near = grp + 1 - 2 * lax.rem(grp, 2)
    far = lax.rem(grp + 2, groups)
    chunk = width // groups
    nb = width // LANES
    batches = min(owners, BATCHES)
    units = owners // batches
    unit_rows = units * rows_per

    barrier = pltpu.get_barrier_semaphore()

    def greet(r, _):
        pl.semaphore_signal(
            barrier, inc=1, device_id=(partner(me, r, owners), grp), device_id_type=MESH
        )
        return 0

    lax.fori_loop(1, owners, greet, 0)
    for peer in (near, far):
        pl.semaphore_signal(barrier, inc=1, device_id=(me, peer), device_id_type=MESH)

    clusters, spots, _ = planes.shape
    points = owner_row.shape[1]
    earlier = (
        lax.broadcasted_iota(jnp.int32, (points, points), 0)
        < lax.broadcasted_iota(jnp.int32, (points, points), 1)
    )
    spread = jnp.broadcast_to(owner_row[...], (points, points))
    ahead = jnp.where((spread.T == spread) & earlier, 1, 0)
    place = owner_row[...] * rows_per + jnp.sum(ahead, axis=0, keepdims=True)
    place = jnp.concatenate([place + capacity * r for r in range(spots // points)], 1)
    slot = lax.broadcasted_iota(jnp.int32, (owners * rows_per, spots), 0)
    pick = jnp.where(slot == place, 1.0, 0.0).astype(send.dtype)

    def pack(k):
        send[k] = mm(pick, planes[k], NN, False).astype(send.dtype)

    def rows_at(i):
        return pl.ds(pl.multiple_of(i * rows_per, rows_per), rows_per)

    def landing(b, side):
        return pl.ds((2 * b + side) * unit_rows, unit_rows)

    def own_copy(k):
        return pltpu.make_async_copy(
            send.at[k, rows_at(me)], rows.at[k, pl.ds(0, rows_per)], own_sem.at[k]
        )

    def issue(k, b):
        def one(i, _):
            r = b * units + i
            to = partner(me, r, owners)
            at = 2 * b * unit_rows + i * rows_per
            pltpu.make_async_remote_copy(
                src_ref=send.at[k, rows_at(to)],
                dst_ref=rows.at[k, pl.ds(pl.multiple_of(at, rows_per), rows_per)],
                send_sem=a_send.at[k], recv_sem=a_recv.at[k, b],
                device_id=(to, grp), device_id_type=MESH,
            ).start()
            return 0

        if b == 0:
            own_copy(k).start()
        if units == 1:
            if b:
                one(0, 0)
        else:
            lax.fori_loop(0 if b else 1, units, one, 0)

    far_copies = {}

    def arrive(k, b):
        remote = unit_rows if b else unit_rows - rows_per
        if remote:
            taken = rows.at[k, pl.ds(0, remote)]
            pltpu.make_async_copy(taken, taken, a_recv.at[k, b]).wait()
        if b == 0:
            own_copy(k).wait()
        copy = pltpu.make_async_remote_copy(
            src_ref=rows.at[k, landing(b, 0)], dst_ref=rows.at[k, landing(b, 1)],
            send_sem=f_send.at[k, b], recv_sem=f_recv.at[k, b],
            device_id=(me, far), device_id_type=MESH,
        )
        copy.start()
        far_copies[k, b] = copy

    def landed(k, some):
        for b in some:
            far_copies[k, b].wait_recv()

    def span(some):
        return slice(2 * some[0] * unit_rows, 2 * (some[-1] + 1) * unit_rows)

    half = -(-2 * chunk // LANES) * LANES
    start = pl.multiple_of(grp // 2 * (width - half), LANES)

    def add_full(n, left, right, some):
        value = mm(rows[left, span(some), :], rows[right, span(some), :], TN, False)
        part[n] = value if some[0] == 0 else part[n] + value

    def add_window(m, left, right, some):
        value = mm(
            rows[left, span(some), pl.ds(start, half)], rows[right, span(some), :], TN, False
        )
        window[m] = value if some[0] == 0 else window[m] + value

    def full_copy(n):
        return pltpu.make_async_remote_copy(
            src_ref=part.at[n], dst_ref=other.at[n],
            send_sem=n_send.at[n], recv_sem=n_recv.at[n],
            device_id=(me, near), device_id_type=MESH,
        )

    def in_window(g):
        return pl.ds(pl.multiple_of(g * chunk - start, TILE), chunk)

    def window_copy(m):
        return pltpu.make_async_remote_copy(
            src_ref=window.at[m, in_window(near)], dst_ref=chunks.at[m],
            send_sem=w_send.at[m], recv_sem=w_recv.at[m],
            device_id=(me, near), device_id_type=MESH,
        )

    mine = pl.ds(pl.multiple_of(grp * chunk, TILE), chunk)

    def summed(n):
        full_copy(n).wait()
        other[n] = part[n] + other[n]

    def own_chunk(m):
        window_copy(m).wait()
        return window[m, in_window(grp), :] + chunks[m]

    pack(1)
    pl.semaphore_wait(barrier, owners - 1 + 2)
    everything = list(range(batches))
    early, late = everything[: batches // 2], everything[batches // 2 :]
    for b in everything:
        issue(1, b)
    pack(2)
    for b in early:
        arrive(1, b)
        issue(2, b)
    pack(0)
    arrive(2, 0)
    for b in late:
        arrive(1, b)
        issue(2, b)
        if b == late[0]:
            for e in early:
                issue(0, e)
        if b == late[1]:
            landed(1, early)
            add_full(0, 1, 1, early)
    for b in early[1:]:
        arrive(2, b)
    landed(1, late[:-1])
    add_full(0, 1, 1, late[:-1])
    for b in early:
        arrive(0, b)
    for b in late[:2]:
        issue(0, b)
    landed(1, late[-1:])
    add_full(0, 1, 1, late[-1:])
    full_copy(0).start()
    full_copy(0).wait()
    eye = (
        lax.broadcasted_iota(jnp.int32, (LANES, LANES), 0)
        == lax.broadcasted_iota(jnp.int32, (LANES, LANES), 1)
    )
    system[...] = part[0] + other[0]
    for i in range(nb):
        at = slice(i * LANES, (i + 1) * LANES)
        system[at, at] = system[at, at] + jnp.where(eye, damp[:, at], 0.0)

    def grams_high():
        landed(2, everything)
        add_full(1, 2, 1, everything)
        full_copy(1).start()
        add_window(0, 2, 2, everything)
        window_copy(0).start()

    plan = {2: [(2, late[0])], 4: [(2, late[1])], 5: [(2, late[2])], 7: [(2, late[3])], 9: [(0, late[0])], 11: [(0, late[1])]}

    def between(j):
        for k, b in plan.get(j, ()):
            arrive(k, b)
        if j == 2:
            for b in late[2:]:
                issue(0, b)
        if j == 10:
            grams_high()

    invert(system, between)
    summed(1)
    solved_high = mm(other[1, mine, :], system[...], NN, True)
    arrive(0, late[2])
    highs[...] = own_chunk(0) - mm(solved_high, other[1], NT, True)
    carry = pltpu.make_async_remote_copy(
        src_ref=highs, dst_ref=carried, send_sem=c_send, recv_sem=c_recv,
        device_id=(lax.rem(me + 1, owners), grp), device_id_type=MESH,
    )
    carry.start()
    arrive(0, late[3])
    first = everything[:-1]
    for some in (first, everything[-1:]):
        landed(0, some)
        add_full(2, 0, 1, some)
        if some is not first:
            full_copy(2).start()
        add_window(1, 0, 0, some)
        add_window(2, 2, 0, some)
    window_copy(1).start()
    window_copy(2).start()
    summed(2)
    solved_low = mm(other[2, mine, :], system[...], NN, True)
    both = mm(jnp.concatenate([solved_low, solved_high], 0), other[2], NT, True)
    low_out[...] = own_chunk(1) - both[:chunk]
    pair_out[...] = own_chunk(2) - both[chunk:]
    for copy in far_copies.values():
        copy.wait_send()
    for k in range(clusters):
        sent = send.at[k, pl.ds(0, (owners - 1) * rows_per)]
        pltpu.make_async_copy(sent, sent, a_send.at[k]).wait()
    carry.wait()


def finish(low, pair, carried, diag_out, pair_out):
    diag_out[...] = low[...] + carried[...]
    pair_out[...] = pair[...]


def local(jacobian, owner, damping):
    points, clusters, residuals, width = jacobian.shape
    owners = lax.axis_size("pts")
    groups = lax.axis_size("grp")
    capacity = max(2, 2 * points // owners)
    rows_per = -(-residuals * capacity // 16) * 16
    total = owners * rows_per
    planes = jnp.transpose(jacobian, (1, 2, 0, 3)).reshape(clusters, residuals * points, width)
    chunk = width // groups
    half = -(-2 * chunk // LANES) * LANES
    batches = min(owners, BATCHES)
    vmem = pl.BlockSpec(memory_space=pltpu.VMEM)
    dma = pltpu.SemaphoreType.DMA
    low, pair, carried = pl.pallas_call(
        functools.partial(kernel, owners, groups, rows_per, width, capacity),
        out_shape=[jax.ShapeDtypeStruct((chunk, width), jnp.float32)] * 3,
        in_specs=[vmem] * 3,
        out_specs=[vmem] * 3,
        scratch_shapes=[
            pltpu.VMEM((clusters, total, width), jacobian.dtype),
            pltpu.VMEM((clusters, 2 * total, width), jacobian.dtype),
            pltpu.VMEM((width, width), jnp.float32),
            pltpu.VMEM((3, width, width), jnp.float32),
            pltpu.VMEM((3, width, width), jnp.float32),
            pltpu.VMEM((3, half, width), jnp.float32),
            pltpu.VMEM((3, chunk, width), jnp.float32),
            pltpu.VMEM((chunk, width), jnp.float32),
            dma((clusters,)), dma((clusters, batches)), dma((clusters,)),
            dma((clusters, batches)), dma((clusters, batches)),
            dma((3,)), dma((3,)), dma((3,)), dma((3,)),
            dma, dma,
        ],
        compiler_params=pltpu.CompilerParams(collective_id=0, has_side_effects=True),
    )(planes, owner.reshape(1, points), damping)
    diag, pair = pl.pallas_call(
        finish,
        out_shape=[jax.ShapeDtypeStruct((chunk, width), jnp.float32)] * 2,
        in_specs=[vmem] * 3,
        out_specs=[vmem] * 2,
    )(low, pair, carried)
    return diag.T[None], pair.T[None]


def solution(mesh):
    placed = (P(("pts", "grp"), None, None, None), P(("pts", "grp"), None), P("pts", None))
    return jax.shard_map(
        local,
        mesh=mesh,
        in_specs=placed,
        out_specs=(P("pts", None, "grp"), P("pts", None, "grp")),
        check_vma=False,
    )
```

```python
import functools

import jax
import jax.numpy as jnp
from jax import lax
from jax.experimental import pallas as pl
from jax.experimental.pallas import tpu as pltpu
from jax.sharding import PartitionSpec as P

MESH = pl.DeviceIdType.MESH
LANES = 128
TILE = 8
PANEL = 32
BATCHES = 8
RELAYED = 2


def mm(left, right, dims, precise):
    return lax.dot_general(
        left,
        right,
        (dims, ((), ())),
        precision=lax.Precision.HIGHEST if precise else None,
        preferred_element_type=jnp.float32,
    )


NN = ((1,), (0,))
NT = ((1,), (1,))
TN = ((0,), (0,))


def sub_row(tile, r):
    return jnp.broadcast_to(tile[r : r + 1, :], (TILE, LANES))


def sub_lane(tile, c):
    return jnp.broadcast_to(tile[:, c : c + 1], (TILE, LANES))


def invert_panel(tiles, first, group):
    lane = lax.broadcasted_iota(jnp.int32, (TILE, LANES), 1)
    sub = lax.broadcasted_iota(jnp.int32, (TILE, LANES), 0)
    count = len(tiles)
    for tile in range(count):
        start = tile * TILE
        columns = {u: [sub_lane(row[group], first + start + u) for row in tiles] for u in range(TILE)}
        for t in range(TILE):
            at = first + start + t
            here = sub == t
            pivot = columns.pop(t)
            scale = 1.0 / sub_row(pivot[tile], t)
            for u in columns:
                lead = sub_row(columns[u][tile], t) * scale
                columns[u] = [c - p * lead for c, p in zip(columns[u], pivot)]
                columns[u][tile] = jnp.where(here, lead, columns[u][tile])
            for part in range(len(tiles[0])):
                row = sub_row(tiles[tile][part], t) * scale
                if part == group:
                    row = jnp.where(lane == at, scale, row)
                for g in range(count):
                    old = tiles[g][part]
                    if part == group:
                        old = jnp.where(lane == at, 0.0, old)
                    tiles[g][part] = old - pivot[g] * row
                tiles[tile][part] = jnp.where(here, row, tiles[tile][part])
    return tiles


def invert(s, between):
    size = s.shape[0]
    panels = size // PANEL
    lane = lax.broadcasted_iota(jnp.int32, (1, size), 1)

    def tiles_of(value):
        return [
            [value[g : g + TILE, c : c + LANES] for c in range(0, size, LANES)]
            for g in range(0, PANEL, TILE)
        ]

    def updated(j, rows):
        at = slice(j * PANEL, (j + 1) * PANEL)
        kept = jnp.where((lane >= j * PANEL) & (lane < (j + 1) * PANEL), 0.0, s[rows, :])
        return kept - mm(s[rows, at], s[at, :], NN, True)

    def update(j, after):
        for rows in (slice(0, j * PANEL), slice((j + after) * PANEL, size)):
            if rows.stop > rows.start:
                s[rows, :] = updated(j, rows)

    tiles = tiles_of(s[:PANEL, :])
    for j in range(panels):
        between(j)
        if j:
            update(j - 1, 2)
        tiles = invert_panel(tiles, j * PANEL % LANES, j * PANEL // LANES)
        for g in range(PANEL // TILE):
            for c in range(size // LANES):
                s[j * PANEL + g * TILE : j * PANEL + (g + 1) * TILE, c * LANES : (c + 1) * LANES] = tiles[g][c]
        if j + 1 < panels:
            tiles = tiles_of(updated(j, slice((j + 1) * PANEL, (j + 2) * PANEL)))
    update(panels - 1, 1)


def partner(me, r, owners):
    out, bit = 0, 1
    while bit < owners:
        mine, flip = lax.rem(me // bit, 2), (r // bit) % 2
        out = out + bit * (mine + flip - 2 * mine * flip)
        bit *= 2
    return out


def kernel(
    owners, groups, rows_per, width, capacity,
    planes_in, owner_in, damp_in, low_out, pair_out, carried,
    planes, owner_row, damp, send, rows, last, system, part, other, window, chunks, highs,
    in_sem, a_send, a_recv, own_sem, f_send, f_recv, n_send, n_recv, w_send, w_recv, l_send, l_recv, c_send, c_recv,
):
    me = lax.axis_index("pts")
    grp = lax.axis_index("grp")
    near = grp + 1 - 2 * lax.rem(grp, 2)
    far = lax.rem(grp + 2, groups)
    chunk = width // groups
    nb = width // LANES
    batches = min(owners, BATCHES)
    units = owners // batches
    unit_rows = units * rows_per

    fetches = [
        pltpu.make_async_copy(src, dst, in_sem.at[n])
        for n, (src, dst) in enumerate(((owner_in, owner_row), (planes_in, planes), (damp_in, damp)))
    ]
    for fetch in fetches:
        fetch.start()
    barrier = pltpu.get_barrier_semaphore()

    def greet(r, _):
        pl.semaphore_signal(
            barrier, inc=1, device_id=(partner(me, r, owners), grp), device_id_type=MESH
        )
        return 0

    lax.fori_loop(1, owners, greet, 0)
    for peer in (near, far):
        pl.semaphore_signal(barrier, inc=1, device_id=(me, peer), device_id_type=MESH)

    clusters, spots, _ = planes.shape
    points = owner_row.shape[1]
    earlier = (
        lax.broadcasted_iota(jnp.int32, (points, points), 0)
        < lax.broadcasted_iota(jnp.int32, (points, points), 1)
    )
    fetches[0].wait()
    spread = jnp.broadcast_to(owner_row[...], (points, points))
    ahead = jnp.where((spread.T == spread) & earlier, 1, 0)
    place = owner_row[...] * rows_per + jnp.sum(ahead, axis=0, keepdims=True)
    place = jnp.concatenate([place + capacity * r for r in range(spots // points)], 1)
    slot = lax.broadcasted_iota(jnp.int32, (owners * rows_per, spots), 0)
    pick = jnp.where(slot == place, 1.0, 0.0).astype(send.dtype)

    def pack(k):
        send[k] = mm(pick, planes[k], NN, False).astype(send.dtype)

    def rows_at(i):
        return pl.ds(pl.multiple_of(i * rows_per, rows_per), rows_per)

    def landing(b, side):
        return pl.ds((2 * b + side) * unit_rows, unit_rows)

    def own_copy(k):
        return pltpu.make_async_copy(
            send.at[k, rows_at(me)], rows.at[k, pl.ds(0, rows_per)], own_sem.at[k]
        )

    def issue(k, b):
        def one(i, _):
            r = b * units + i
            to = partner(me, r, owners)
            at = 2 * b * unit_rows + i * rows_per
            pltpu.make_async_remote_copy(
                src_ref=send.at[k, rows_at(to)],
                dst_ref=rows.at[k, pl.ds(pl.multiple_of(at, rows_per), rows_per)],
                send_sem=a_send.at[k], recv_sem=a_recv.at[k, b],
                device_id=(to, grp), device_id_type=MESH,
            ).start()
            return 0

        if b == 0:
            own_copy(k).start()
        if units == 1:
            if b:
                one(0, 0)
        else:
            lax.fori_loop(0 if b else 1, units, one, 0)

    far_copies = {}

    def arrive(k, b):
        remote = unit_rows if b else unit_rows - rows_per
        if remote:
            taken = rows.at[k, pl.ds(0, remote)]
            pltpu.make_async_copy(taken, taken, a_recv.at[k, b]).wait()
        if b == 0:
            own_copy(k).wait()
        copy = pltpu.make_async_remote_copy(
            src_ref=rows.at[k, landing(b, 0)], dst_ref=rows.at[k, landing(b, 1)],
            send_sem=f_send.at[k, b], recv_sem=f_recv.at[k, b],
            device_id=(me, far), device_id_type=MESH,
        )
        copy.start()
        far_copies[k, b] = copy
        if b >= batches - RELAYED:
            relay(k, b, 0).start()

    def relay(k, b, side):
        at = (2 * (b - batches + RELAYED) + side) * unit_rows
        return pltpu.make_async_remote_copy(
            src_ref=rows.at[k, landing(b, side)], dst_ref=last.at[k, pl.ds(at, unit_rows)],
            send_sem=l_send.at[k, b, side], recv_sem=l_recv.at[k, b, side],
            device_id=(me, near), device_id_type=MESH,
        )

    def landed(k, some):
        for b in some:
            far_copies[k, b].wait_recv()
            if b >= batches - RELAYED:
                relay(k, b, 1).start()

    def span(some):
        return slice(2 * some[0] * unit_rows, 2 * (some[-1] + 1) * unit_rows)

    half = -(-2 * chunk // LANES) * LANES
    start = pl.multiple_of(grp // 2 * (width - half), LANES)

    def add_full(n, left, right, some):
        value = mm(rows[left, span(some), :], rows[right, span(some), :], TN, False)
        part[n] = value if some[0] == 0 else part[n] + value

    def add_window(m, left, right, some):
        value = mm(
            rows[left, span(some), pl.ds(start, half)], rows[right, span(some), :], TN, False
        )
        window[m] = value if some[0] == 0 else window[m] + value

    def full_copy(n):
        return pltpu.make_async_remote_copy(
            src_ref=part.at[n], dst_ref=other.at[n],
            send_sem=n_send.at[n], recv_sem=n_recv.at[n],
            device_id=(me, near), device_id_type=MESH,
        )

    def in_window(g):
        return pl.ds(pl.multiple_of(g * chunk - start, TILE), chunk)

    def window_copy(m):
        return pltpu.make_async_remote_copy(
            src_ref=window.at[m, in_window(near)], dst_ref=chunks.at[m],
            send_sem=w_send.at[m], recv_sem=w_recv.at[m],
            device_id=(me, near), device_id_type=MESH,
        )

    mine = pl.ds(pl.multiple_of(grp * chunk, TILE), chunk)

    def summed(n):
        full_copy(n).wait()
        other[n] = part[n] + other[n]

    def own_chunk(m):
        window_copy(m).wait()
        return window[m, in_window(grp), :] + chunks[m]

    fetches[1].wait()
    fetches[2].wait()
    pack(1)
    pl.semaphore_wait(barrier, owners - 1 + 2)
    everything = list(range(batches))
    early, late = everything[: batches // 2], everything[batches // 2 :]
    for b in everything:
        issue(1, b)
    arrive(1, 0)
    pack(2)
    issue(2, 0)
    for b in early[1:]:
        arrive(1, b)
        issue(2, b)
    arrive(2, 0)
    pack(0)
    for b in late:
        arrive(1, b)
        issue(2, b)
        if b == late[1]:
            for e in early:
                issue(0, e)
            landed(1, early)
            add_full(0, 1, 1, early)
    first, tail = everything[: batches - RELAYED], everything[batches - RELAYED :]
    ends = span(tail)
    columns = pl.ds(start, half)

    def relayed(k):
        for b in tail:
            for side in range(2):
                relay(k, b, side).wait()

    rest = [b for b in first if b not in early]
    landed(1, rest)
    add_full(0, 1, 1, rest)
    full_copy(0).start()
    for b in early[1:]:
        arrive(2, b)
    landed(1, tail)
    system[...] = mm(rows[1, ends, :], rows[1, ends, :], TN, False)
    full_copy(0).wait()
    system[...] = system[...] + (part[0] + other[0])
    relayed(1)
    system[...] = system[...] + mm(last[1], last[1], TN, False)
    eye = (
        lax.broadcasted_iota(jnp.int32, (LANES, LANES), 0)
        == lax.broadcasted_iota(jnp.int32, (LANES, LANES), 1)
    )
    for i in range(nb):
        at = slice(i * LANES, (i + 1) * LANES)
        system[at, at] = system[at, at] + jnp.where(eye, damp[:, at], 0.0)

    plan = {
        0: [(0, e) for e in early[:2]], 1: [(0, early[2])], 2: [(0, early[3])],
        3: [(2, late[0])], 4: [(2, late[1])], 5: [(2, late[2])], 7: [(2, late[3])],
        9: [(0, late[0])], 11: [(0, late[1])],
    }
    sends = {0: late[0], 2: late[1], 3: late[2], 4: late[3]}

    def between(j):
        for k, b in plan.get(j, ()):
            arrive(k, b)
        if j in sends:
            issue(0, sends[j])
        if j == 9:
            landed(2, first)
            add_full(1, 2, 1, first)
            full_copy(1).start()
            add_window(0, 2, 2, first)
            window_copy(0).start()
        if j == 11:
            landed(2, tail)

    invert(system, between)
    arrive(0, late[2])
    summed(1)
    relayed(2)
    other[1] = other[1] + (
        mm(rows[2, ends, :], rows[1, ends, :], TN, False) + mm(last[2], last[1], TN, False)
    )
    solved_high = mm(other[1, mine, :], system[...], NN, True)
    arrive(0, late[3])
    chunks[0] = own_chunk(0)
    window[0] = mm(rows[2, ends, columns], rows[2, ends, :], TN, False) + mm(
        last[2, :, columns], last[2], TN, False
    )
    highs[...] = chunks[0] + window[0, in_window(grp), :] - mm(solved_high, other[1], NT, True)
    carry = pltpu.make_async_remote_copy(
        src_ref=highs, dst_ref=carried, send_sem=c_send, recv_sem=c_recv,
        device_id=(lax.rem(me + 1, owners), grp), device_id_type=MESH,
    )
    carry.start()
    landed(0, first)
    add_full(2, 0, 1, first)
    full_copy(2).start()
    add_window(1, 0, 0, first)
    window_copy(1).start()
    add_window(2, 2, 0, first)
    window_copy(2).start()
    landed(0, tail[:-1])
    summed(2)
    for m in (1, 2):
        chunks[m] = own_chunk(m)
    landed(0, tail[-1:])
    other[2] = other[2] + mm(rows[0, ends, :], rows[1, ends, :], TN, False)
    for m, k in ((1, 0), (2, 2)):
        window[m] = mm(rows[k, ends, columns], rows[0, ends, :], TN, False)
    relayed(0)
    other[2] = other[2] + mm(last[0], last[1], TN, False)
    solved_low = mm(other[2, mine, :], system[...], NN, True)
    for m, k in ((1, 0), (2, 2)):
        window[m] = window[m] + mm(last[k, :, columns], last[0], TN, False)
    both = mm(jnp.concatenate([solved_low, solved_high], 0), other[2], NT, True)
    low_out[...] = chunks[1] + window[1, in_window(grp), :] - both[:chunk]
    pair_out[...] = chunks[2] + window[2, in_window(grp), :] - both[chunk:]
    for copy in far_copies.values():
        copy.wait_send()
    for k in range(clusters):
        sent = send.at[k, pl.ds(0, (owners - 1) * rows_per)]
        pltpu.make_async_copy(sent, sent, a_send.at[k]).wait()
    carry.wait()


def finish(low, pair, carried, diag_out, pair_out):
    diag_out[...] = low[...] + carried[...]
    pair_out[...] = pair[...]


def local(jacobian, owner, damping):
    points, clusters, residuals, width = jacobian.shape
    owners = lax.axis_size("pts")
    groups = lax.axis_size("grp")
    capacity = max(2, 2 * points // owners)
    rows_per = -(-residuals * capacity // 16) * 16
    total = owners * rows_per
    planes = jnp.transpose(jacobian, (1, 2, 0, 3)).reshape(clusters, residuals * points, width)
    chunk = width // groups
    half = -(-2 * chunk // LANES) * LANES
    batches = min(owners, BATCHES)
    vmem = pl.BlockSpec(memory_space=pltpu.VMEM)
    dma = pltpu.SemaphoreType.DMA
    low, pair, carried = pl.pallas_call(
        functools.partial(kernel, owners, groups, rows_per, width, capacity),
        out_shape=[jax.ShapeDtypeStruct((chunk, width), jnp.float32)] * 3,
        in_specs=[pl.BlockSpec(memory_space=pl.ANY)] * 3,
        out_specs=[vmem] * 3,
        scratch_shapes=[
            pltpu.VMEM(planes.shape, planes.dtype),
            pltpu.VMEM((1, points), owner.dtype),
            pltpu.VMEM(damping.shape, damping.dtype),
            pltpu.VMEM((clusters, total, width), jacobian.dtype),
            pltpu.VMEM((clusters, 2 * total, width), jacobian.dtype),
            pltpu.VMEM((clusters, 2 * RELAYED * total // batches, width), jacobian.dtype),
            pltpu.VMEM((width, width), jnp.float32),
            pltpu.VMEM((3, width, width), jnp.float32),
            pltpu.VMEM((3, width, width), jnp.float32),
            pltpu.VMEM((3, half, width), jnp.float32),
            pltpu.VMEM((3, chunk, width), jnp.float32),
            pltpu.VMEM((chunk, width), jnp.float32),
            dma((3,)), dma((clusters,)), dma((clusters, batches)), dma((clusters,)),
            dma((clusters, batches)), dma((clusters, batches)),
            dma((3,)), dma((3,)), dma((3,)), dma((3,)),
            dma((clusters, batches, 2)), dma((clusters, batches, 2)), dma, dma,
        ],
        compiler_params=pltpu.CompilerParams(collective_id=0, has_side_effects=True),
    )(planes, owner.reshape(1, points), damping)
    diag, pair = pl.pallas_call(
        finish,
        out_shape=[jax.ShapeDtypeStruct((chunk, width), jnp.float32)] * 2,
        in_specs=[vmem] * 3,
        out_specs=[vmem] * 2,
    )(low, pair, carried)
    return diag.T[None], pair.T[None]


def solution(mesh):
    placed = (P(("pts", "grp"), None, None, None), P(("pts", "grp"), None), P("pts", None))
    return jax.shard_map(
        local,
        mesh=mesh,
        in_specs=placed,
        out_specs=(P("pts", None, "grp"), P("pts", None, "grp")),
        check_vma=False,
    )
```

```python
import functools

import jax
import jax.numpy as jnp
from jax import lax
from jax.experimental import pallas as pl
from jax.experimental.pallas import tpu as pltpu
from jax.sharding import PartitionSpec as P

MESH = pl.DeviceIdType.MESH
LANES = 128
TILE = 8
PANEL = 32
BATCHES = 8
RELAYED = 2


def mm(left, right, dims, precise):
    return lax.dot_general(
        left,
        right,
        (dims, ((), ())),
        precision=lax.Precision.HIGHEST if precise else None,
        preferred_element_type=jnp.float32,
    )


NN = ((1,), (0,))
NT = ((1,), (1,))
TN = ((0,), (0,))


def sub_row(tile, r):
    return jnp.broadcast_to(tile[r : r + 1, :], (TILE, LANES))


def sub_lane(tile, c):
    return jnp.broadcast_to(tile[:, c : c + 1], (TILE, LANES))


def invert_panel(tiles, first, group):
    lane = lax.broadcasted_iota(jnp.int32, (TILE, LANES), 1)
    sub = lax.broadcasted_iota(jnp.int32, (TILE, LANES), 0)
    count = len(tiles)
    for tile in range(count):
        start = tile * TILE
        columns = {u: [sub_lane(row[group], first + start + u) for row in tiles] for u in range(TILE)}
        for t in range(TILE):
            at = first + start + t
            here = sub == t
            pivot = columns.pop(t)
            scale = 1.0 / sub_row(pivot[tile], t)
            for u in columns:
                lead = sub_row(columns[u][tile], t) * scale
                columns[u] = [c - p * lead for c, p in zip(columns[u], pivot)]
                columns[u][tile] = jnp.where(here, lead, columns[u][tile])
            for part in range(len(tiles[0])):
                row = sub_row(tiles[tile][part], t) * scale
                if part == group:
                    row = jnp.where(lane == at, scale, row)
                for g in range(count):
                    old = tiles[g][part]
                    if part == group:
                        old = jnp.where(lane == at, 0.0, old)
                    tiles[g][part] = old - pivot[g] * row
                tiles[tile][part] = jnp.where(here, row, tiles[tile][part])
    return tiles


def invert(s, between):
    size = s.shape[0]
    panels = size // PANEL
    lane = lax.broadcasted_iota(jnp.int32, (1, size), 1)

    def tiles_of(value):
        return [
            [value[g : g + TILE, c : c + LANES] for c in range(0, size, LANES)]
            for g in range(0, PANEL, TILE)
        ]

    def updated(j, rows):
        at = slice(j * PANEL, (j + 1) * PANEL)
        kept = jnp.where((lane >= j * PANEL) & (lane < (j + 1) * PANEL), 0.0, s[rows, :])
        return kept - mm(s[rows, at], s[at, :], NN, True)

    def update(j, after):
        for rows in (slice(0, j * PANEL), slice((j + after) * PANEL, size)):
            if rows.stop > rows.start:
                s[rows, :] = updated(j, rows)

    tiles = tiles_of(s[:PANEL, :])
    for j in range(panels):
        between(j)
        if j:
            update(j - 1, 2)
        tiles = invert_panel(tiles, j * PANEL % LANES, j * PANEL // LANES)
        for g in range(PANEL // TILE):
            for c in range(size // LANES):
                s[j * PANEL + g * TILE : j * PANEL + (g + 1) * TILE, c * LANES : (c + 1) * LANES] = tiles[g][c]
        if j + 1 < panels:
            tiles = tiles_of(updated(j, slice((j + 1) * PANEL, (j + 2) * PANEL)))
    update(panels - 1, 1)


def partner(me, r, owners):
    out, bit = 0, 1
    while bit < owners:
        mine, flip = lax.rem(me // bit, 2), (r // bit) % 2
        out = out + bit * (mine + flip - 2 * mine * flip)
        bit *= 2
    return out


def kernel(
    owners, groups, rows_per, width, capacity,
    planes_in, owner_in, damp_in, low_out, pair_out, carried,
    planes, owner_row, damp, send, rows, last, system, part, other, window, chunks, highs,
    in_sem, a_send, a_recv, own_sem, f_send, f_recv, n_send, n_recv, w_send, w_recv, l_send, l_recv, c_send, c_recv,
):
    me = lax.axis_index("pts")
    grp = lax.axis_index("grp")
    near = grp + 1 - 2 * lax.rem(grp, 2)
    far = lax.rem(grp + 2, groups)
    chunk = width // groups
    nb = width // LANES
    batches = min(owners, BATCHES)
    units = owners // batches
    unit_rows = units * rows_per

    fetches = [
        pltpu.make_async_copy(src, dst, in_sem.at[n])
        for n, (src, dst) in enumerate(((owner_in, owner_row), (planes_in, planes), (damp_in, damp)))
    ]
    for fetch in fetches:
        fetch.start()
    barrier = pltpu.get_barrier_semaphore()

    def greet(r, _):
        pl.semaphore_signal(
            barrier, inc=1, device_id=(partner(me, r, owners), grp), device_id_type=MESH
        )
        return 0

    lax.fori_loop(1, owners, greet, 0)
    for peer in (near, far):
        pl.semaphore_signal(barrier, inc=1, device_id=(me, peer), device_id_type=MESH)

    clusters, spots, _ = planes.shape
    points = owner_row.shape[1]
    earlier = (
        lax.broadcasted_iota(jnp.int32, (points, points), 0)
        < lax.broadcasted_iota(jnp.int32, (points, points), 1)
    )
    fetches[0].wait()
    spread = jnp.broadcast_to(owner_row[...], (points, points))
    ahead = jnp.where((spread.T == spread) & earlier, 1, 0)
    place = owner_row[...] * rows_per + jnp.sum(ahead, axis=0, keepdims=True)
    place = jnp.concatenate([place + capacity * r for r in range(spots // points)], 1)
    slot = lax.broadcasted_iota(jnp.int32, (owners * rows_per, spots), 0)
    pick = jnp.where(slot == place, 1.0, 0.0).astype(send.dtype)

    def pack(k):
        send[k] = mm(pick, planes[k], NN, False).astype(send.dtype)

    def rows_at(i):
        return pl.ds(pl.multiple_of(i * rows_per, rows_per), rows_per)

    def landing(b, side):
        return pl.ds((2 * b + side) * unit_rows, unit_rows)

    def own_copy(k):
        return pltpu.make_async_copy(
            send.at[k, rows_at(me)], rows.at[k, pl.ds(0, rows_per)], own_sem.at[k]
        )

    def issue(k, b):
        def one(i, _):
            r = b * units + i
            to = partner(me, r, owners)
            at = 2 * b * unit_rows + i * rows_per
            pltpu.make_async_remote_copy(
                src_ref=send.at[k, rows_at(to)],
                dst_ref=rows.at[k, pl.ds(pl.multiple_of(at, rows_per), rows_per)],
                send_sem=a_send.at[k], recv_sem=a_recv.at[k, b],
                device_id=(to, grp), device_id_type=MESH,
            ).start()
            return 0

        if b == 0:
            own_copy(k).start()
        if units == 1:
            if b:
                one(0, 0)
        else:
            lax.fori_loop(0 if b else 1, units, one, 0)

    far_copies = {}

    def arrive(k, b):
        remote = unit_rows if b else unit_rows - rows_per
        if remote:
            taken = rows.at[k, pl.ds(0, remote)]
            pltpu.make_async_copy(taken, taken, a_recv.at[k, b]).wait()
        if b == 0:
            own_copy(k).wait()
        copy = pltpu.make_async_remote_copy(
            src_ref=rows.at[k, landing(b, 0)], dst_ref=rows.at[k, landing(b, 1)],
            send_sem=f_send.at[k, b], recv_sem=f_recv.at[k, b],
            device_id=(me, far), device_id_type=MESH,
        )
        copy.start()
        far_copies[k, b] = copy
        if b >= batches - RELAYED:
            relay(k, b, 0).start()

    def relay(k, b, side):
        at = (2 * (b - batches + RELAYED) + side) * unit_rows
        return pltpu.make_async_remote_copy(
            src_ref=rows.at[k, landing(b, side)], dst_ref=last.at[k, pl.ds(at, unit_rows)],
            send_sem=l_send.at[k, b, side], recv_sem=l_recv.at[k, b, side],
            device_id=(me, near), device_id_type=MESH,
        )

    def landed(k, some):
        for b in some:
            far_copies[k, b].wait_recv()
            if b >= batches - RELAYED:
                relay(k, b, 1).start()

    def span(some):
        return slice(2 * some[0] * unit_rows, 2 * (some[-1] + 1) * unit_rows)

    half = -(-2 * chunk // LANES) * LANES
    start = pl.multiple_of(grp // 2 * (width - half), LANES)

    def add_full(n, left, right, some):
        value = mm(rows[left, span(some), :], rows[right, span(some), :], TN, False)
        part[n] = value if some[0] == 0 else part[n] + value

    def add_window(m, left, right, some):
        value = mm(
            rows[left, span(some), pl.ds(start, half)], rows[right, span(some), :], TN, False
        )
        window[m] = value if some[0] == 0 else window[m] + value

    def full_copy(n):
        return pltpu.make_async_remote_copy(
            src_ref=part.at[n], dst_ref=other.at[n],
            send_sem=n_send.at[n], recv_sem=n_recv.at[n],
            device_id=(me, near), device_id_type=MESH,
        )

    def in_window(g):
        return pl.ds(pl.multiple_of(g * chunk - start, TILE), chunk)

    def window_copy(m):
        return pltpu.make_async_remote_copy(
            src_ref=window.at[m, in_window(near)], dst_ref=chunks.at[m],
            send_sem=w_send.at[m], recv_sem=w_recv.at[m],
            device_id=(me, near), device_id_type=MESH,
        )

    mine = pl.ds(pl.multiple_of(grp * chunk, TILE), chunk)

    def summed(n):
        full_copy(n).wait()
        other[n] = part[n] + other[n]

    def own_chunk(m):
        window_copy(m).wait()
        return window[m, in_window(grp), :] + chunks[m]

    fetches[1].wait()
    fetches[2].wait()
    pack(1)
    pl.semaphore_wait(barrier, owners - 1 + 2)
    everything = list(range(batches))
    early, late = everything[: batches // 2], everything[batches // 2 :]
    for b in everything:
        issue(1, b)
    arrive(1, 0)
    pack(2)
    issue(2, 0)
    for b in early[1:]:
        arrive(1, b)
        issue(2, b)
    arrive(2, 0)
    pack(0)
    for b in late:
        arrive(1, b)
        issue(2, b)
        if b == late[1]:
            for e in early:
                issue(0, e)
            landed(1, early)
            add_full(0, 1, 1, early)
    first, tail = everything[: batches - RELAYED], everything[batches - RELAYED :]
    ends = span(tail)
    columns = pl.ds(start, half)

    def relayed(k):
        for b in tail:
            for side in range(2):
                relay(k, b, side).wait()

    rest = [b for b in first if b not in early]
    landed(1, rest)
    add_full(0, 1, 1, rest)
    full_copy(0).start()
    for b in early[1:]:
        arrive(2, b)
    landed(1, tail)
    system[...] = mm(rows[1, ends, :], rows[1, ends, :], TN, False)
    full_copy(0).wait()
    system[...] = system[...] + (part[0] + other[0])
    relayed(1)
    system[...] = system[...] + mm(last[1], last[1], TN, False)
    eye = (
        lax.broadcasted_iota(jnp.int32, (LANES, LANES), 0)
        == lax.broadcasted_iota(jnp.int32, (LANES, LANES), 1)
    )
    for i in range(nb):
        at = slice(i * LANES, (i + 1) * LANES)
        system[at, at] = system[at, at] + jnp.where(eye, damp[:, at], 0.0)

    plan = {
        0: [(0, e) for e in early[:2]], 1: [(0, early[2])], 2: [(0, early[3])],
        3: [(2, late[0])], 4: [(2, late[1])], 5: [(2, late[2])], 7: [(2, late[3])],
        9: [(0, late[0])], 11: [(0, late[1])],
    }
    sends = {1: late[0], 3: late[1], 4: late[2], 5: late[3]}

    def between(j):
        for k, b in plan.get(j, ()):
            arrive(k, b)
        if j in sends:
            issue(0, sends[j])
        if j == 8:
            landed(2, first)
            add_full(1, 2, 1, first)
            full_copy(1).start()
            add_window(0, 2, 2, first)
            window_copy(0).start()
        if j == 11:
            landed(2, tail)

    invert(system, between)
    arrive(0, late[2])
    summed(1)
    relayed(2)
    other[1] = other[1] + (
        mm(rows[2, ends, :], rows[1, ends, :], TN, False) + mm(last[2], last[1], TN, False)
    )
    solved_high = mm(other[1, mine, :], system[...], NN, True)
    arrive(0, late[3])
    chunks[0] = own_chunk(0)
    window[0] = mm(rows[2, ends, columns], rows[2, ends, :], TN, False) + mm(
        last[2, :, columns], last[2], TN, False
    )
    highs[...] = chunks[0] + window[0, in_window(grp), :] - mm(solved_high, other[1], NT, True)
    carry = pltpu.make_async_remote_copy(
        src_ref=highs, dst_ref=carried, send_sem=c_send, recv_sem=c_recv,
        device_id=(lax.rem(me + 1, owners), grp), device_id_type=MESH,
    )
    carry.start()
    landed(0, first)
    add_full(2, 0, 1, first)
    full_copy(2).start()
    add_window(1, 0, 0, first)
    window_copy(1).start()
    add_window(2, 2, 0, first)
    window_copy(2).start()
    landed(0, tail[:-1])
    summed(2)
    for m in (1, 2):
        chunks[m] = own_chunk(m)
    landed(0, tail[-1:])
    other[2] = other[2] + mm(rows[0, ends, :], rows[1, ends, :], TN, False)
    for m, k in ((1, 0), (2, 2)):
        window[m] = mm(rows[k, ends, columns], rows[0, ends, :], TN, False)
    relayed(0)
    other[2] = other[2] + mm(last[0], last[1], TN, False)
    solved_low = mm(other[2, mine, :], system[...], NN, True)
    for m, k in ((1, 0), (2, 2)):
        window[m] = window[m] + mm(last[k, :, columns], last[0], TN, False)
    both = mm(jnp.concatenate([solved_low, solved_high], 0), other[2], NT, True)
    low_out[...] = chunks[1] + window[1, in_window(grp), :] - both[:chunk]
    pair_out[...] = chunks[2] + window[2, in_window(grp), :] - both[chunk:]
    for copy in far_copies.values():
        copy.wait_send()
    for k in range(clusters):
        sent = send.at[k, pl.ds(0, (owners - 1) * rows_per)]
        pltpu.make_async_copy(sent, sent, a_send.at[k]).wait()
    carry.wait()


def finish(low, pair, carried, diag_out, pair_out):
    diag_out[...] = low[...] + carried[...]
    pair_out[...] = pair[...]


def local(jacobian, owner, damping):
    points, clusters, residuals, width = jacobian.shape
    owners = lax.axis_size("pts")
    groups = lax.axis_size("grp")
    capacity = max(2, 2 * points // owners)
    rows_per = -(-residuals * capacity // 16) * 16
    total = owners * rows_per
    planes = jnp.transpose(jacobian, (1, 2, 0, 3)).reshape(clusters, residuals * points, width)
    chunk = width // groups
    half = -(-2 * chunk // LANES) * LANES
    batches = min(owners, BATCHES)
    vmem = pl.BlockSpec(memory_space=pltpu.VMEM)
    dma = pltpu.SemaphoreType.DMA
    low, pair, carried = pl.pallas_call(
        functools.partial(kernel, owners, groups, rows_per, width, capacity),
        out_shape=[jax.ShapeDtypeStruct((chunk, width), jnp.float32)] * 3,
        in_specs=[pl.BlockSpec(memory_space=pl.ANY)] * 3,
        out_specs=[vmem] * 3,
        scratch_shapes=[
            pltpu.VMEM(planes.shape, planes.dtype),
            pltpu.VMEM((1, points), owner.dtype),
            pltpu.VMEM(damping.shape, damping.dtype),
            pltpu.VMEM((clusters, total, width), jacobian.dtype),
            pltpu.VMEM((clusters, 2 * total, width), jacobian.dtype),
            pltpu.VMEM((clusters, 2 * RELAYED * total // batches, width), jacobian.dtype),
            pltpu.VMEM((width, width), jnp.float32),
            pltpu.VMEM((3, width, width), jnp.float32),
            pltpu.VMEM((3, width, width), jnp.float32),
            pltpu.VMEM((3, half, width), jnp.float32),
            pltpu.VMEM((3, chunk, width), jnp.float32),
            pltpu.VMEM((chunk, width), jnp.float32),
            dma((3,)), dma((clusters,)), dma((clusters, batches)), dma((clusters,)),
            dma((clusters, batches)), dma((clusters, batches)),
            dma((3,)), dma((3,)), dma((3,)), dma((3,)),
            dma((clusters, batches, 2)), dma((clusters, batches, 2)), dma, dma,
        ],
        compiler_params=pltpu.CompilerParams(collective_id=0, has_side_effects=True),
    )(planes, owner.reshape(1, points), damping)
    diag, pair = pl.pallas_call(
        finish,
        out_shape=[jax.ShapeDtypeStruct((chunk, width), jnp.float32)] * 2,
        in_specs=[vmem] * 3,
        out_specs=[vmem] * 2,
    )(low, pair, carried)
    return diag.T[None], pair.T[None]


def solution(mesh):
    placed = (P(("pts", "grp"), None, None, None), P(("pts", "grp"), None), P("pts", None))
    return jax.shard_map(
        local,
        mesh=mesh,
        in_specs=placed,
        out_specs=(P("pts", None, "grp"), P("pts", None, "grp")),
        check_vma=False,
    )
```
